32 devices in a mesh: slab: 16 (over z, x, core), layer: 2 (over y).
Axes of the slice: x: 2, y: 2, z: 4, core: 2. Of those that a mesh axis runs over, the one named last changes fastest.
Arguments:
- nodal_field: float32 [2, 1024, 4, 4, 512], P('layer', 'slab'), may hold values from -6 to 6
- metric: float32 [2, 1024, 4, 4, 3, 512], P('layer', 'slab'), may hold values from 0.25 to 2
- slab_ids: int32 [1024], replicated, may hold values from 0 to 1023, as said below
- face_map: int32 [1024, 1024], P('slab'), may hold values from 0 to 1023, as said below
Outputs:
- assembled: float32 [2, 1024, 4, 4, 512], P('layer', 'slab')
The draws below stay inside these ranges and needn't reach their ends.
Inputs may be any that keep to these rules, and one draw needn't show every extreme that they name: slab_ids is a permutation of 0 to 1023; positions p of one device are those with p // 64 equal to its index along slab, and for one rotation R every device holds exactly the slabs g with (g + R) mod 16 equal to its index, in any order of its positions, so slab (g + 1) mod 1024 always sits on the next device along slab, cyclically. Each row of face_map is a permutation of 0 to 1023: either the identity, or the map that reverses y, sending (ez, ey, c, b) to (ez, 3 - ey, c, 7 - b); z order is never changed.
All inputs are finite; a program needn't handle non-finite values.
Results may differ from the reference program's by a relative error of at most 0.00005.
Values sent between devices are 32-bit elements; how exact they have to be, the bound alone decides.
A program may use at most 192 MiB of HBM per device.

```python
import math
import jax
import jax.numpy as jnp
import numpy as np
from jax import lax

P_SIZE = 8
PTS = 512
EY = 4
EZ = 4
SLAB_DEV = 64
FACE = 1024
SLABS = 1024
LAYERS = 2
N_SLAB = 16


def permute_slots(sub_key):
    return jax.random.permutation(sub_key, SLAB_DEV)


def draw_slab_ids(key, part):
    rotate_key = jax.random.fold_in(key, 11)
    order_key = jax.random.fold_in(key, 12)
    rotation = jax.random.randint(rotate_key, (), 0, N_SLAB)
    key_list = jax.random.split(order_key, N_SLAB)
    slot_orders = jax.vmap(permute_slots)(key_list).astype(jnp.int32)
    residues = (jnp.arange(N_SLAB, dtype=jnp.int32) - rotation + N_SLAB) % N_SLAB
    return (slot_orders * N_SLAB + residues[:, None]).reshape(SLABS).astype(jnp.int32)


def draw_face_map(key, part):
    flip_key = jax.random.fold_in(key, 21)
    flip_bits = jax.random.randint(flip_key, (SLABS, 1), 0, 2)
    point_index = jnp.arange(FACE, dtype=jnp.int32)
    column = point_index % P_SIZE
    element_col = point_index // (P_SIZE * P_SIZE) % EY
    reversed_index = point_index + (P_SIZE - 1 - 2 * column) + (EY - 1 - 2 * element_col) * P_SIZE * P_SIZE
    return jnp.where(flip_bits == 1, reversed_index[None, :], point_index[None, :]).astype(jnp.int32)


def steps_of(rng, dims, shards, low, high):
    loudness, own = 1.0, jax.random.fold_in(rng, 6)
    for position, parts in shards:
        steps = jnp.exp(jax.random.uniform(jax.random.fold_in(own, position), (parts,), jnp.float32, low / len(shards), high / len(shards)))
        loudness = loudness * jnp.repeat(steps, dims[position] // parts).reshape([-1 if axis == position else 1 for axis in range(len(dims))])
    return loudness


def noise(key, shape, spread, limit, cuts=(), kind=jnp.bfloat16):
    drawn = spread * jax.random.normal(key, shape, jnp.float32)
    if cuts:
        drawn = drawn * steps_of(key, shape, cuts, -0.22, 0.18)
    return jnp.clip(drawn, -limit, limit).astype(kind)


def setup_inputs(seed: int = 0) -> dict:
    arg_keys = jax.random.split(jax.random.key(seed), 5)
    nodal_field = noise(arg_keys[0], (LAYERS, SLABS, EZ, EY, PTS), 1.0, 6.0, ((0, 2), (1, 16)), jnp.float32)
    metric = jnp.clip(jnp.exp(math.log(2.0) - 2.0794415 * jax.random.uniform(arg_keys[1], (LAYERS, SLABS, EZ, EY, 3, PTS), jnp.float32) ** steps_of(arg_keys[1], (LAYERS, SLABS, EZ, EY, 3, PTS), ((0, 2), (1, 16)), -0.2, 0.2)), 0.25, 2.0)
    slab_ids = draw_slab_ids(jax.random.fold_in(arg_keys[4], 71), 0)
    face_map = draw_face_map(jax.random.fold_in(arg_keys[4], 71), 0)
    return dict(nodal_field=nodal_field, metric=metric, slab_ids=slab_ids, face_map=face_map)


def legendre_pair(gll_nodes, degree):
    lower_poly = gll_nodes * 0.0 + 1.0
    upper_poly = gll_nodes.copy()
    for poly_order in range(2, degree + 1):
        lower_poly, upper_poly = upper_poly, ((2 * poly_order - 1) * gll_nodes * upper_poly - (poly_order - 1) * lower_poly) / poly_order
    return lower_poly, upper_poly


def gll_tables():
    degree = P_SIZE - 1
    gll_nodes = -np.cos(np.pi * np.arange(P_SIZE) / degree)
    for newton_sweep in range(100):
        lower_poly, upper_poly = legendre_pair(gll_nodes, degree)
        gll_nodes = gll_nodes - (gll_nodes * upper_poly - lower_poly) / ((degree + 1) * upper_poly)
    lower_poly, upper_poly = legendre_pair(gll_nodes, degree)
    quad_weights = 2.0 / (degree * (degree + 1) * upper_poly * upper_poly)
    identity = np.eye(P_SIZE)
    differ = gll_nodes[:, None] - gll_nodes[None, :] + identity
    derivative = upper_poly[:, None] / (upper_poly[None, :] * differ)
    derivative = derivative * (1.0 - identity)
    derivative[0, 0] = -degree * (degree + 1) / 4.0
    derivative[degree, degree] = degree * (degree + 1) / 4.0
    weight_cube = quad_weights[:, None, None] * quad_weights[None, :, None] * quad_weights[None, None, :]
    return jnp.asarray(derivative, jnp.float32), jnp.asarray(weight_cube, jnp.float32)


def local_apply(values, factors, derivative, weight_cube):
    highest = lax.Precision.HIGHEST
    grad_x = jnp.einsum("ai,...cbi->...cba", derivative, values, precision=highest)
    grad_y = jnp.einsum("bi,...cia->...cba", derivative, values, precision=highest)
    grad_z = jnp.einsum("ci,...iba->...cba", derivative, values, precision=highest)
    flux_x = weight_cube * factors[..., 0, :, :, :] * grad_x
    flux_y = weight_cube * factors[..., 1, :, :, :] * grad_y
    flux_z = weight_cube * factors[..., 2, :, :, :] * grad_z
    result = jnp.einsum("ia,...cbi->...cba", derivative, flux_x, precision=highest)
    result = result + jnp.einsum("ib,...cia->...cba", derivative, flux_y, precision=highest)
    result = result + jnp.einsum("ic,...iba->...cba", derivative, flux_z, precision=highest)
    return result


def assemble_slab(values):
    shared = values[..., :, :-1, :, P_SIZE - 1, :] + values[..., :, 1:, :, 0, :]
    values = values.at[..., :, :-1, :, P_SIZE - 1, :].set(shared)
    values = values.at[..., :, 1:, :, 0, :].set(shared)
    shared = values[..., :-1, :, P_SIZE - 1, :, :] + values[..., 1:, :, 0, :, :]
    values = values.at[..., :-1, :, P_SIZE - 1, :, :].set(shared)
    values = values.at[..., 1:, :, 0, :, :].set(shared)
    return values


def face_of(local_out, column):
    return local_out[..., column].reshape(local_out.shape[:-5] + (FACE,))


def put_face(local_out, face_values, column):
    return local_out.at[..., column].set(face_values.reshape(local_out.shape[:-1]))


def reference(nodal_field, metric, slab_ids, face_map):
    derivative, weight_cube = gll_tables()
    values = nodal_field.reshape(LAYERS * N_SLAB, SLAB_DEV, EZ, EY, P_SIZE, P_SIZE, P_SIZE)
    factors = metric.reshape(LAYERS * N_SLAB, SLAB_DEV, EZ, EY, 3, P_SIZE, P_SIZE, P_SIZE)

    def slab_block(pair_in):
        return assemble_slab(local_apply(pair_in[0], pair_in[1], derivative, weight_cube))

    local_out = lax.map(slab_block, (values, factors)).reshape(LAYERS, SLABS, EZ, EY, P_SIZE, P_SIZE, P_SIZE)
    slab_iota = jnp.arange(SLABS, dtype=jnp.int32)
    inverse = jnp.zeros((SLABS,), jnp.int32).at[slab_ids].set(slab_iota)
    next_pos = inverse[(slab_ids + 1) % SLABS]
    prev_pos = inverse[(slab_ids + SLABS - 1) % SLABS]
    right_face = face_of(local_out, P_SIZE - 1)
    left_face = face_of(local_out, 0)
    reoriented = jnp.zeros_like(right_face).at[:, slab_iota[:, None], face_map].set(right_face)
    left_sum = left_face + reoriented[:, prev_pos]
    right_sum = right_face + jnp.take_along_axis(left_face[:, next_pos], face_map[None, :, :], axis=2)
    local_out = put_face(local_out, left_sum, 0)
    local_out = put_face(local_out, right_sum, P_SIZE - 1)
    top_face = local_out[:, :, EZ - 1, :, P_SIZE - 1, :, :]
    bottom_face = local_out[:, :, 0, :, 0, :, :]
    top_sum = top_face + jnp.roll(bottom_face, -1, axis=0)
    bottom_sum = bottom_face + jnp.roll(top_face, 1, axis=0)
    local_out = local_out.at[:, :, 0, :, 0, :, :].set(bottom_sum)
    local_out = local_out.at[:, :, EZ - 1, :, P_SIZE - 1, :, :].set(top_sum)
    return local_out.reshape(LAYERS, SLABS, EZ, EY, PTS)
```

```python
import functools

import jax
import jax.numpy as jnp
import numpy as np
from jax import lax
from jax.experimental import pallas as pl
from jax.experimental.pallas import tpu as pltpu
from jax.sharding import PartitionSpec as P

P_SIZE = 8
PTS = 512
EY = 4
EZ = 4
SUB = 8
LANES = 128


def legendre_pair(nodes, degree):
    lower = nodes * 0.0 + 1.0
    upper = nodes.copy()
    for order in range(2, degree + 1):
        lower, upper = upper, ((2 * order - 1) * nodes * upper - (order - 1) * lower) / order
    return lower, upper


def gll_tables():
    degree = P_SIZE - 1
    nodes = -np.cos(np.pi * np.arange(P_SIZE) / degree)
    for _ in range(100):
        lower, upper = legendre_pair(nodes, degree)
        nodes = nodes - (nodes * upper - lower) / ((degree + 1) * upper)
    lower, upper = legendre_pair(nodes, degree)
    rho = 2.0 / (degree * (degree + 1) * upper * upper)
    eye = np.eye(P_SIZE)
    differ = nodes[:, None] - nodes[None, :] + eye
    der = upper[:, None] / (upper[None, :] * differ) * (1.0 - eye)
    der[0, 0] = -degree * (degree + 1) / 4.0
    der[degree, degree] = degree * (degree + 1) / 4.0
    return der, rho


def two_parts(table):
    high = np.asarray(table, np.float32).astype(jnp.bfloat16)
    low = (table - high.astype(np.float64)).astype(jnp.bfloat16)
    return high, low


def tables():
    der, rho = gll_tables()
    eye8, eye2 = np.eye(8), np.eye(2)
    plane = np.tile(np.kron(rho, rho), 2)
    fwd = np.concatenate(
        [np.kron(np.eye(16), der.T) * plane, np.kron(eye2, np.kron(der.T, eye8)) * plane], 1
    )
    high, low = two_parts(fwd)
    fwd_op = np.concatenate([high, high, low], 0)
    bwd = np.concatenate([np.kron(np.eye(16), der), np.kron(eye2, np.kron(der, eye8))], 0)
    high, low = two_parts(bwd)
    half = np.concatenate([high, low], 1)
    bwd_op = np.concatenate([half, half], 0)
    l2 = (np.arange(SUB) // EY)[:, None]
    h = (np.arange(LANES) // 64)[None, :]
    cube_plane = plane[None, :]
    zf = np.zeros((2, 2, 2, 2, SUB, LANES))
    zb = np.zeros((2, 2, 2, 2, SUB, LANES))
    rc = np.zeros((2, SUB, LANES))
    for lo in range(2):
        c_out = 2 * (2 * lo + l2) + h
        rc[lo] = rho[c_out]
        for li in range(2):
            for s in range(2):
                for l in range(2):
                    c_in = 2 * (2 * li + (l2 ^ s)) + (h ^ l)
                    zf[lo, li, s, l] = der[c_out, c_in] * rho[c_out] * cube_plane
                    zb[lo, li, s, l] = der[c_in, c_out]
    consts = np.concatenate([zf.reshape(-1, SUB, LANES), zb.reshape(-1, SUB, LANES), rc], 0)
    return fwd_op, bwd_op, consts.astype(np.float32)


def roll_sub(x, by):
    return pltpu.roll(x, by % SUB, axis=x.ndim - 2)


def roll_lane(x, by):
    return pltpu.roll(x, by % LANES, axis=x.ndim - 1)


def split(x):
    high = x.astype(jnp.bfloat16)
    return high, (x - high.astype(jnp.float32)).astype(jnp.bfloat16)


def iotas():
    sub = lax.broadcasted_iota(jnp.int32, (SUB, LANES), 0)
    lane = lax.broadcasted_iota(jnp.int32, (SUB, LANES), 1)
    return sub, lane


def lane_gather(x, index):
    return jnp.take_along_axis(x, index, axis=1, mode="promise_in_bounds")


def flip(x, sub, lane):
    y = lane_gather(x, lane ^ 7)
    e = sub % EY
    return jnp.where(
        e == 0, roll_sub(y, -3), jnp.where(e == 1, roll_sub(y, -1), jnp.where(e == 2, roll_sub(y, 1), roll_sub(y, 3)))
    )


def apply_z(pair, consts, base):
    terms = []
    for v in pair:
        sv = roll_sub(v, 4)
        terms += [v, roll_lane(v, 64), sv, roll_lane(sv, 64)]
    out = []
    for lo in range(2):
        acc = consts[base + 8 * lo] * terms[0]
        for t in range(1, 8):
            acc = acc + consts[base + 8 * lo + t] * terms[t]
        out.append(acc)
    return out


def slab_work(sb, u_ref, m_ref, fm_ref, fwd_ref, bwd_ref, consts, put_v, put_faces):
    rows = sb * 64
    u = u_ref[...]
    high, low = split(u)
    g = jnp.dot(
        jnp.concatenate([high, low, high], 1), fwd_ref[...], preferred_element_type=jnp.float32
    )
    m = m_ref[...].reshape(sb * EZ, 3, 16, LANES)
    gx = g[:, :LANES].reshape(sb * EZ, 16, LANES)
    gy = g[:, LANES:].reshape(sb * EZ, 16, LANES)
    fx = (gx * m[:, 0]).reshape(rows, LANES)
    fy = (gy * m[:, 1]).reshape(rows, LANES)
    xh, xl = split(fx)
    yh, yl = split(fy)
    r = jnp.dot(
        jnp.concatenate([xh, yh, xl, yl], 1), bwd_ref[...], preferred_element_type=jnp.float32
    )
    r = (r[:, :LANES] + r[:, LANES:]).reshape(sb * EZ, 2, SUB, LANES)
    u4 = u.reshape(sb * EZ, 2, SUB, LANES)
    mz = m[:, 2].reshape(sb * EZ, 2, SUB, LANES)
    sub, lane = iotas()
    ey, b = sub % EY, lane // 8 % 8
    mask_up = (ey < EY - 1) & (b == 7)
    mask_dn = (ey > 0) & (b == 0)
    top_mask = (sub >= 4) & (lane >= 64)
    bot_mask = (sub < 4) & (lane < 64)
    group = lane // 16
    pick = (lane % 16) * 8
    edges = [None, None]
    z_hold = None
    for s in range(sb):
        v = []
        for ez in range(EZ):
            i = s * EZ + ez
            gz = apply_z([u4[i, 0], u4[i, 1]], consts, 0)
            out = apply_z([gz[0] * mz[i, 0], gz[1] * mz[i, 1]], consts, 16)
            for t in range(2):
                w = out[t] + consts[32 + t] * r[i, t]
                up = roll_lane(roll_sub(w, -1), 56)
                dn = roll_lane(roll_sub(w, 1), -56)
                v.append(w + jnp.where(mask_up, up, 0.0) + jnp.where(mask_dn, dn, 0.0))
        for ez in range(EZ - 1):
            a, c = v[2 * ez + 1], v[2 * ez + 2]
            v[2 * ez + 1] = a + jnp.where(top_mask, roll_lane(roll_sub(c, 4), 64), 0.0)
            v[2 * ez + 2] = c + jnp.where(bot_mask, roll_lane(roll_sub(a, 4), 64), 0.0)
        left = jnp.zeros((SUB, LANES), jnp.float32)
        right = left
        for k in range(8):
            put_v(s, k, v[k])
            left = jnp.where(group == k, lane_gather(v[k], pick), left)
            right = jnp.where(group == k, lane_gather(v[k], pick + 7), right)
        flag = jnp.broadcast_to(fm_ref[s : s + 1, 0:1], (SUB, LANES)) != 0
        right = jnp.where(flag, flip(right, sub, lane), right)
        put_faces(0, s, right)
        put_faces(1, s, left)
        for side, face in enumerate((right, left)):
            edge = roll_sub(jnp.where(sub < 4, face, roll_lane(face, 8)), 4)
            edge = roll_lane(edge, 8 * s) if s else edge
            edges[side] = edge if s == 0 else jnp.where(lane // 8 == s, edge, edges[side])
        z = jnp.where(sub < 4, v[0], v[7])
        if s % 2 == 0:
            z_hold = z
        else:
            put_faces(2, s // 2, jnp.where((sub < 4) == (lane < 64), z_hold, roll_lane(z, 64)))
    put_faces(3, 0, edges[0])
    put_faces(4, 0, edges[1])


def local_kernel(sb, u_ref, m_ref, fm_ref, fwd_ref, bwd_ref, consts, v_ref, pr_ref, pl_ref, z_ref, er_ref, el_ref):
    faces = (pr_ref, pl_ref, z_ref, er_ref, el_ref)

    def put_v(s, k, value):
        v_ref[pl.ds(s * 64 + k * 8, 8), :] = value

    def put_faces(which, at, value):
        faces[which][at] = value

    slab_work(sb, u_ref, m_ref, fm_ref, fwd_ref, bwd_ref, consts, put_v, put_faces)


def finish_kernel(
    sb, slabs, peers, ids_ref, v_ref, fm_ref, pr_ref, pl_ref, z_ref, er_ref, el_ref, out_ref, inv_ref
):
    step = pl.program_id(0)
    me = lax.axis_index("slab")
    total = slabs * peers
    behind = lax.rem(me + peers - 1, peers) * slabs
    ahead = lax.rem(me + 1, peers) * slabs

    @pl.when(step == 0)
    def _():
        for p in range(slabs):
            inv_ref[0, ids_ref[behind + p] // peers] = p
            inv_ref[1, ids_ref[ahead + p] // peers] = p

    sub, lane = iotas()
    top_mask = (sub >= 4) & (lane >= 64)
    bot_mask = (sub < 4) & (lane < 64)
    a = lane % 8
    spread = lane // 8

    def edge_of(ref, q):
        e = pltpu.roll(ref[q // sb], (LANES - 8 * (q % sb)) % LANES, axis=1)
        return jnp.where(
            (sub < 4) & (lane < 8), e, jnp.where((sub >= 4) & (lane >= 120), roll_lane(e, -8), 0.0)
        )

    for s in range(sb):
        own = ids_ref[me * slabs + step * sb + s]
        q_prev = inv_ref[0, lax.rem(own + total - 1, total) // peers]
        q_next = inv_ref[1, lax.rem(own + 1, total) // peers]
        left = pr_ref[q_prev] + edge_of(er_ref, q_prev)
        right = pl_ref[q_next] + edge_of(el_ref, q_next)
        flag = jnp.broadcast_to(fm_ref[s : s + 1, 0:1], (SUB, LANES)) != 0
        right = jnp.where(flag, flip(right, sub, lane), right)
        z = z_ref[s // 2]
        if s % 2:
            z = roll_lane(z, 64)
        z = roll_lane(roll_sub(z, 4), 64)
        for k in range(8):
            add = jnp.where(
                a == 0,
                lane_gather(left, spread + 16 * k),
                jnp.where(a == 7, lane_gather(right, spread + 16 * k), 0.0),
            )
            w = v_ref[pl.ds(s * 64 + k * 8, 8), :] + add
            if k == 0:
                w = w + jnp.where(bot_mask, z, 0.0)
            if k == 7:
                w = w + jnp.where(top_mask, z, 0.0)
            out_ref[pl.ds(s * 64 + k * 8, 8), :] = w


def body(sb, peers, nodal_field, metric, slab_ids, face_map):
    slabs = nodal_field.shape[1]
    steps = slabs // sb
    fwd_op, bwd_op, consts = tables()
    u = nodal_field.reshape(slabs, EZ, EY, 4, LANES).transpose(0, 1, 3, 2, 4).reshape(slabs * 64, LANES)
    m = (
        metric.reshape(slabs, EZ, EY, 3, 4, LANES)
        .transpose(0, 1, 3, 4, 2, 5)
        .reshape(slabs * 192, LANES)
    )
    f32 = jnp.float32
    whole = lambda shape: pl.BlockSpec(shape, lambda i: (0,) * len(shape))
    stack = lambda n: pl.BlockSpec((n, SUB, LANES), lambda i: (i, 0, 0))
    v, pr, plf, z, er, el = pl.pallas_call(
        functools.partial(local_kernel, sb),
        grid=(steps,),
        in_specs=[
            pl.BlockSpec((sb * 64, LANES), lambda i: (i, 0)),
            pl.BlockSpec((sb * 192, LANES), lambda i: (i, 0)),
            pl.BlockSpec((sb, LANES), lambda i: (i, 0)),
            whole(fwd_op.shape),
            whole(bwd_op.shape),
            whole(consts.shape),
        ],
        out_specs=[
            pl.BlockSpec((sb * 64, LANES), lambda i: (i, 0)),
            stack(sb),
            stack(sb),
            stack(sb // 2),
            stack(1),
            stack(1),
        ],
        out_shape=[
            jax.ShapeDtypeStruct((slabs * 64, LANES), f32),
            jax.ShapeDtypeStruct((slabs, SUB, LANES), f32),
            jax.ShapeDtypeStruct((slabs, SUB, LANES), f32),
            jax.ShapeDtypeStruct((slabs // 2, SUB, LANES), f32),
            jax.ShapeDtypeStruct((steps, SUB, LANES), f32),
            jax.ShapeDtypeStruct((steps, SUB, LANES), f32),
        ],
        name="local",
    )(u, m, face_map, jnp.asarray(fwd_op), jnp.asarray(bwd_op), jnp.asarray(consts))
    ring = [(i, (i + 1) % peers) for i in range(peers)]
    back = [(j, i) for i, j in ring]
    both = lambda pairs: [(2 * i + l, 2 * j + 1 - l) for i, j in pairs for l in range(2)]
    pr = lax.ppermute(pr, "slab", ring)
    plf = lax.ppermute(plf, "slab", back)
    z = lax.ppermute(z, "layer", [(0, 1), (1, 0)])
    er = lax.ppermute(er, ("slab", "layer"), both(ring))
    el = lax.ppermute(el, ("slab", "layer"), both(back))
    out = pl.pallas_call(
        functools.partial(finish_kernel, sb, slabs, peers),
        grid=(steps,),
        in_specs=[
            pl.BlockSpec(memory_space=pltpu.SMEM),
            pl.BlockSpec((sb * 64, LANES), lambda i: (i, 0)),
            pl.BlockSpec((sb, LANES), lambda i: (i, 0)),
            whole((slabs, SUB, LANES)),
            whole((slabs, SUB, LANES)),
            stack(sb // 2),
            whole((steps, SUB, LANES)),
            whole((steps, SUB, LANES)),
        ],
        out_specs=pl.BlockSpec((sb * 64, LANES), lambda i: (i, 0)),
        out_shape=jax.ShapeDtypeStruct((slabs * 64, LANES), f32),
        scratch_shapes=[pltpu.SMEM((2, slabs), jnp.int32)],
        name="finish",
    )(slab_ids, v, face_map, pr, plf, z, er, el)
    out = out.reshape(slabs, EZ, 4, EY, LANES).transpose(0, 1, 3, 2, 4)
    return out.reshape(1, slabs, EZ, EY, PTS)


def solution(mesh):
    return jax.shard_map(
        functools.partial(body, 8, mesh.shape["slab"]),
        mesh=mesh,
        in_specs=(
            P("layer", "slab", None, None, None),
            P("layer", "slab", None, None, None, None),
            P(),
            P("slab", None),
        ),
        out_specs=P("layer", "slab", None, None, None),
        check_vma=False,
    )
```

```python
import functools

import jax
import jax.numpy as jnp
import numpy as np
from jax import lax
from jax.experimental import pallas as pl
from jax.experimental.pallas import tpu as pltpu
from jax.sharding import PartitionSpec as P

P_SIZE = 8
PTS = 512
EY = 4
EZ = 4
SUB = 8
LANES = 128


def legendre_pair(nodes, degree):
    lower = nodes * 0.0 + 1.0
    upper = nodes.copy()
    for order in range(2, degree + 1):
        lower, upper = upper, ((2 * order - 1) * nodes * upper - (order - 1) * lower) / order
    return lower, upper


def gll_tables():
    degree = P_SIZE - 1
    nodes = -np.cos(np.pi * np.arange(P_SIZE) / degree)
    for _ in range(100):
        lower, upper = legendre_pair(nodes, degree)
        nodes = nodes - (nodes * upper - lower) / ((degree + 1) * upper)
    lower, upper = legendre_pair(nodes, degree)
    rho = 2.0 / (degree * (degree + 1) * upper * upper)
    eye = np.eye(P_SIZE)
    differ = nodes[:, None] - nodes[None, :] + eye
    der = upper[:, None] / (upper[None, :] * differ) * (1.0 - eye)
    der[0, 0] = -degree * (degree + 1) / 4.0
    der[degree, degree] = degree * (degree + 1) / 4.0
    return der, rho


def two_parts(table):
    high = np.asarray(table, np.float32).astype(jnp.bfloat16)
    low = (table - high.astype(np.float64)).astype(jnp.bfloat16)
    return high, low


def tables():
    der, rho = gll_tables()
    eye8, eye2 = np.eye(8), np.eye(2)
    plane = np.tile(np.kron(rho, rho), 2)
    fwd = np.concatenate(
        [np.kron(np.eye(16), der.T) * plane, np.kron(eye2, np.kron(der.T, eye8)) * plane], 1
    )
    high, low = two_parts(fwd)
    fwd_op = np.concatenate([high, high, low], 0)
    bwd = np.concatenate([np.kron(np.eye(16), der), np.kron(eye2, np.kron(der, eye8))], 0)
    high, low = two_parts(bwd)
    half = np.concatenate([high, low], 1)
    bwd_op = np.concatenate([half, half], 0)
    l2 = (np.arange(SUB) // EY)[:, None]
    h = (np.arange(LANES) // 64)[None, :]
    cube_plane = plane[None, :]
    zf = np.zeros((2, 2, 2, 2, SUB, LANES))
    zb = np.zeros((2, 2, 2, 2, SUB, LANES))
    rc = np.zeros((2, SUB, LANES))
    for lo in range(2):
        c_out = 2 * (2 * lo + l2) + h
        rc[lo] = rho[c_out]
        for li in range(2):
            for s in range(2):
                for l in range(2):
                    c_in = 2 * (2 * li + (l2 ^ s)) + (h ^ l)
                    zf[lo, li, s, l] = der[c_out, c_in] * rho[c_out] * cube_plane
                    zb[lo, li, s, l] = der[c_in, c_out]
    consts = np.concatenate([zf.reshape(-1, SUB, LANES), zb.reshape(-1, SUB, LANES), rc], 0)
    return fwd_op, bwd_op, consts.astype(np.float32)


def roll_sub(x, by):
    return pltpu.roll(x, by % SUB, axis=x.ndim - 2)


def roll_lane(x, by):
    return pltpu.roll(x, by % LANES, axis=x.ndim - 1)


def split(x):
    high = x.astype(jnp.bfloat16)
    return high, (x - high.astype(jnp.float32)).astype(jnp.bfloat16)


def iotas():
    sub = lax.broadcasted_iota(jnp.int32, (SUB, LANES), 0)
    lane = lax.broadcasted_iota(jnp.int32, (SUB, LANES), 1)
    return sub, lane


def lane_gather(x, index):
    return jnp.take_along_axis(x, index, axis=1, mode="promise_in_bounds")


def flip(x, sub, lane):
    y = lane_gather(x, lane ^ 7)
    e = sub % EY
    return jnp.where(
        e == 0, roll_sub(y, -3), jnp.where(e == 1, roll_sub(y, -1), jnp.where(e == 2, roll_sub(y, 1), roll_sub(y, 3)))
    )


def apply_z(pair, consts, base):
    terms = []
    for v in pair:
        sv = roll_sub(v, 4)
        terms += [v, roll_lane(v, 64), sv, roll_lane(sv, 64)]
    out = []
    for lo in range(2):
        acc = consts[base + 8 * lo] * terms[0]
        for t in range(1, 8):
            acc = acc + consts[base + 8 * lo + t] * terms[t]
        out.append(acc)
    return out


def slab_work(sb, u_ref, m_ref, fm_ref, fwd_ref, bwd_ref, consts, put_v, put_faces):
    rows = sb * 64
    u = u_ref[...]
    high, low = split(u)
    g = jnp.dot(
        jnp.concatenate([high, low, high], 1), fwd_ref[...], preferred_element_type=jnp.float32
    )
    m = m_ref[...].reshape(sb * EZ, 3, 16, LANES)
    gx = g[:, :LANES].reshape(sb * EZ, 16, LANES)
    gy = g[:, LANES:].reshape(sb * EZ, 16, LANES)
    fx = (gx * m[:, 0]).reshape(rows, LANES)
    fy = (gy * m[:, 1]).reshape(rows, LANES)
    xh, xl = split(fx)
    yh, yl = split(fy)
    r = jnp.dot(
        jnp.concatenate([xh, yh, xl, yl], 1), bwd_ref[...], preferred_element_type=jnp.float32
    )
    r = (r[:, :LANES] + r[:, LANES:]).reshape(sb * EZ, 2, SUB, LANES)
    u4 = u.reshape(sb * EZ, 2, SUB, LANES)
    mz = m[:, 2].reshape(sb * EZ, 2, SUB, LANES)
    sub, lane = iotas()
    ey, b = sub % EY, lane // 8 % 8
    mask_up = (ey < EY - 1) & (b == 7)
    mask_dn = (ey > 0) & (b == 0)
    top_mask = (sub >= 4) & (lane >= 64)
    bot_mask = (sub < 4) & (lane < 64)
    group = lane // 16
    pick = (lane % 16) * 8
    edges = [None, None]
    z_hold = None
    for s in range(sb):
        v = []
        for ez in range(EZ):
            i = s * EZ + ez
            gz = apply_z([u4[i, 0], u4[i, 1]], consts, 0)
            out = apply_z([gz[0] * mz[i, 0], gz[1] * mz[i, 1]], consts, 16)
            for t in range(2):
                w = out[t] + consts[32 + t] * r[i, t]
                up = roll_lane(roll_sub(w, -1), 56)
                dn = roll_lane(roll_sub(w, 1), -56)
                v.append(w + jnp.where(mask_up, up, 0.0) + jnp.where(mask_dn, dn, 0.0))
        for ez in range(EZ - 1):
            a, c = v[2 * ez + 1], v[2 * ez + 2]
            v[2 * ez + 1] = a + jnp.where(top_mask, roll_lane(roll_sub(c, 4), 64), 0.0)
            v[2 * ez + 2] = c + jnp.where(bot_mask, roll_lane(roll_sub(a, 4), 64), 0.0)
        left = jnp.zeros((SUB, LANES), jnp.float32)
        right = left
        for k in range(8):
            put_v(s, k, v[k])
            left = jnp.where(group == k, lane_gather(v[k], pick), left)
            right = jnp.where(group == k, lane_gather(v[k], pick + 7), right)
        flag = jnp.broadcast_to(fm_ref[s : s + 1, 0:1], (SUB, LANES)) != 0
        right = jnp.where(flag, flip(right, sub, lane), right)
        put_faces(0, s, right)
        put_faces(1, s, left)
        for side, face in enumerate((right, left)):
            edge = roll_sub(jnp.where(sub < 4, face, roll_lane(face, 8)), 4)
            edge = roll_lane(edge, 8 * s) if s else edge
            edges[side] = edge if s == 0 else jnp.where(lane // 8 == s, edge, edges[side])
        z = jnp.where(sub < 4, v[0], v[7])
        if s % 2 == 0:
            z_hold = z
        else:
            put_faces(2, s // 2, jnp.where((sub < 4) == (lane < 64), z_hold, roll_lane(z, 64)))
    put_faces(3, 0, edges[0])
    put_faces(4, 0, edges[1])


def local_kernel(
    sb, steps, peers, u_ref, m_ref, fm_ref, fwd_ref, bwd_ref, consts,
    v_ref, *refs
):
    landing, sending, (send_sem, recv_sem) = refs[:5], refs[5:10], refs[10:]
    step = pl.program_id(0)
    me, layer = lax.axis_index("slab"), lax.axis_index("layer")
    right, left = lax.rem(me + 1, peers), lax.rem(me + peers - 1, peers)
    targets = (
        {"slab": right, "layer": layer},
        {"slab": left, "layer": layer},
        {"slab": me, "layer": 1 - layer},
        {"slab": right, "layer": 1 - layer},
        {"slab": left, "layer": 1 - layer},
    )
    sizes = (sb, sb, sb // 2, 1, 1)
    barrier = pltpu.get_barrier_semaphore()

    def copy_of(which, at):
        rows = pl.ds(at * sizes[which], sizes[which])
        return pltpu.make_async_remote_copy(
            src_ref=sending[which].at[rows],
            dst_ref=landing[which].at[rows],
            send_sem=send_sem.at[which, at],
            recv_sem=recv_sem.at[which, at],
            device_id=targets[which],
            device_id_type=pl.DeviceIdType.MESH,
        )

    @pl.when(step == 0)
    def _():
        for target in targets:
            pl.semaphore_signal(
                barrier, inc=1, device_id=target, device_id_type=pl.DeviceIdType.MESH
            )

    @pl.when(step == 1)
    def _():
        pl.semaphore_wait(barrier, 5)

    @pl.when(step > 0)
    def _():
        for which in range(5):
            copy_of(which, step - 1).start()

    def put_v(s, k, value):
        v_ref[pl.ds(s * 64 + k * 8, 8), :] = value

    def put_faces(which, at, value):
        sending[which][step * sizes[which] + at] = value

    slab_work(sb, u_ref, m_ref, fm_ref, fwd_ref, bwd_ref, consts, put_v, put_faces)

    @pl.when(step == steps - 1)
    def _():
        def drain(at, carry):
            for which in range(5):
                copy_of(which, at).wait_send()
            return carry

        def collect(at, carry):
            for which in range(5):
                copy_of(which, at).wait_recv()
            return carry

        lax.fori_loop(0, steps - 1, drain, 0)
        for which in range(5):
            copy_of(which, steps - 1).start()
        drain(steps - 1, 0)
        lax.fori_loop(0, steps, collect, 0)


def finish_kernel(
    sb, slabs, peers, ids_ref, v_ref, fm_ref, pr_ref, pl_ref, z_ref, er_ref, el_ref, out_ref, inv_ref
):
    step = pl.program_id(0)
    me = lax.axis_index("slab")
    total = slabs * peers
    behind = lax.rem(me + peers - 1, peers) * slabs
    ahead = lax.rem(me + 1, peers) * slabs

    @pl.when(step == 0)
    def _():
        for p in range(slabs):
            inv_ref[0, lax.div(ids_ref[behind + p], peers)] = p
            inv_ref[1, lax.div(ids_ref[ahead + p], peers)] = p

    sub, lane = iotas()
    top_mask = (sub >= 4) & (lane >= 64)
    bot_mask = (sub < 4) & (lane < 64)
    a = lane % 8
    spread = lane // 8

    def edge_of(ref, q):
        e = pltpu.roll(ref[lax.div(q, sb)], LANES - 8 * lax.rem(q, sb), axis=1)
        return jnp.where(
            (sub < 4) & (lane < 8), e, jnp.where((sub >= 4) & (lane >= 120), roll_lane(e, -8), 0.0)
        )

    for s in range(sb):
        own = ids_ref[me * slabs + step * sb + s]
        q_prev = inv_ref[0, lax.div(lax.rem(own + total - 1, total), peers)]
        q_next = inv_ref[1, lax.div(lax.rem(own + 1, total), peers)]
        left = pr_ref[q_prev] + edge_of(er_ref, q_prev)
        right = pl_ref[q_next] + edge_of(el_ref, q_next)
        flag = jnp.broadcast_to(fm_ref[s : s + 1, 0:1], (SUB, LANES)) != 0
        right = jnp.where(flag, flip(right, sub, lane), right)
        z = z_ref[s // 2]
        if s % 2:
            z = roll_lane(z, 64)
        z = roll_lane(roll_sub(z, 4), 64)
        for k in range(8):
            add = jnp.where(
                a == 0,
                lane_gather(left, spread + 16 * k),
                jnp.where(a == 7, lane_gather(right, spread + 16 * k), 0.0),
            )
            w = v_ref[pl.ds(s * 64 + k * 8, 8), :] + add
            if k == 0:
                w = w + jnp.where(bot_mask, z, 0.0)
            if k == 7:
                w = w + jnp.where(top_mask, z, 0.0)
            out_ref[pl.ds(s * 64 + k * 8, 8), :] = w


def body(sb, peers, nodal_field, metric, slab_ids, face_map):
    slabs = nodal_field.shape[1]
    steps = slabs // sb
    fwd_op, bwd_op, consts = tables()
    u = nodal_field.reshape(slabs, EZ, EY, 4, LANES).transpose(0, 1, 3, 2, 4).reshape(slabs * 64, LANES)
    m = (
        metric.reshape(slabs, EZ, EY, 3, 4, LANES)
        .transpose(0, 1, 3, 4, 2, 5)
        .reshape(slabs * 192, LANES)
    )
    f32 = jnp.float32
    whole = lambda shape: pl.BlockSpec(shape, lambda i: (0,) * len(shape))
    stack = lambda n: pl.BlockSpec((n, SUB, LANES), lambda i: (i, 0, 0))
    v, pr, plf, z, er, el = pl.pallas_call(
        functools.partial(local_kernel, sb, steps, peers),
        grid=(steps,),
        in_specs=[
            pl.BlockSpec((sb * 64, LANES), lambda i: (i, 0)),
            pl.BlockSpec((sb * 192, LANES), lambda i: (i, 0)),
            pl.BlockSpec((sb, LANES), lambda i: (i, 0)),
            whole(fwd_op.shape),
            whole(bwd_op.shape),
            whole(consts.shape),
        ],
        out_specs=[
            pl.BlockSpec((sb * 64, LANES), lambda i: (i, 0)),
            *[pl.BlockSpec(memory_space=pl.ANY)] * 5,
        ],
        out_shape=[
            jax.ShapeDtypeStruct((slabs * 64, LANES), f32),
            jax.ShapeDtypeStruct((slabs, SUB, LANES), f32),
            jax.ShapeDtypeStruct((slabs, SUB, LANES), f32),
            jax.ShapeDtypeStruct((slabs // 2, SUB, LANES), f32),
            jax.ShapeDtypeStruct((steps, SUB, LANES), f32),
            jax.ShapeDtypeStruct((steps, SUB, LANES), f32),
        ],
        scratch_shapes=[
            pltpu.VMEM((slabs, SUB, LANES), f32),
            pltpu.VMEM((slabs, SUB, LANES), f32),
            pltpu.VMEM((slabs // 2, SUB, LANES), f32),
            pltpu.VMEM((steps, SUB, LANES), f32),
            pltpu.VMEM((steps, SUB, LANES), f32),
            pltpu.SemaphoreType.DMA((5, steps)),
            pltpu.SemaphoreType.DMA((5, steps)),
        ],
        compiler_params=pltpu.CompilerParams(collective_id=0, has_side_effects=True),
        name="local",
    )(u, m, face_map, jnp.asarray(fwd_op), jnp.asarray(bwd_op), jnp.asarray(consts))
    out = pl.pallas_call(
        functools.partial(finish_kernel, sb, slabs, peers),
        grid=(steps,),
        in_specs=[
            pl.BlockSpec(memory_space=pltpu.SMEM),
            pl.BlockSpec((sb * 64, LANES), lambda i: (i, 0)),
            pl.BlockSpec((sb, LANES), lambda i: (i, 0)),
            whole((slabs, SUB, LANES)),
            whole((slabs, SUB, LANES)),
            stack(sb // 2),
            whole((steps, SUB, LANES)),
            whole((steps, SUB, LANES)),
        ],
        out_specs=pl.BlockSpec((sb * 64, LANES), lambda i: (i, 0)),
        out_shape=jax.ShapeDtypeStruct((slabs * 64, LANES), f32),
        scratch_shapes=[pltpu.SMEM((2, slabs), jnp.int32)],
        name="finish",
    )(slab_ids, v, face_map, pr, plf, z, er, el)
    out = out.reshape(slabs, EZ, 4, EY, LANES).transpose(0, 1, 3, 2, 4)
    return out.reshape(1, slabs, EZ, EY, PTS)


def solution(mesh):
    return jax.shard_map(
        functools.partial(body, 8, mesh.shape["slab"]),
        mesh=mesh,
        in_specs=(
            P("layer", "slab", None, None, None),
            P("layer", "slab", None, None, None, None),
            P(),
            P("slab", None),
        ),
        out_specs=P("layer", "slab", None, None, None),
        check_vma=False,
    )
```

```python
import functools

import jax
import jax.numpy as jnp
import numpy as np
from jax import lax
from jax.experimental import pallas as pl
from jax.experimental.pallas import tpu as pltpu
from jax.sharding import PartitionSpec as P

P_SIZE = 8
PTS = 512
EY = 4
EZ = 4
SUB = 8
LANES = 128
SB = 8
SBF = 16


def legendre_pair(nodes, degree):
    lower = nodes * 0.0 + 1.0
    upper = nodes.copy()
    for order in range(2, degree + 1):
        lower, upper = upper, ((2 * order - 1) * nodes * upper - (order - 1) * lower) / order
    return lower, upper


def gll_tables():
    degree = P_SIZE - 1
    nodes = -np.cos(np.pi * np.arange(P_SIZE) / degree)
    for _ in range(100):
        lower, upper = legendre_pair(nodes, degree)
        nodes = nodes - (nodes * upper - lower) / ((degree + 1) * upper)
    lower, upper = legendre_pair(nodes, degree)
    rho = 2.0 / (degree * (degree + 1) * upper * upper)
    eye = np.eye(P_SIZE)
    differ = nodes[:, None] - nodes[None, :] + eye
    der = upper[:, None] / (upper[None, :] * differ) * (1.0 - eye)
    der[0, 0] = -degree * (degree + 1) / 4.0
    der[degree, degree] = degree * (degree + 1) / 4.0
    return der, rho


def two_parts(table):
    high = np.asarray(table, np.float32).astype(jnp.bfloat16)
    low = (table - high.astype(np.float64)).astype(jnp.bfloat16)
    return high, low


def tables():
    der, rho = gll_tables()
    eye8, eye2 = np.eye(8), np.eye(2)
    plane = np.tile(np.kron(rho, rho), 2)
    fwd = np.concatenate(
        [np.kron(np.eye(16), der.T) * plane, np.kron(eye2, np.kron(der.T, eye8)) * plane], 1
    )
    high, low = two_parts(fwd)
    fwd_op = np.concatenate([high, high, low], 0)
    bwd = np.concatenate([np.kron(np.eye(16), der), np.kron(eye2, np.kron(der, eye8))], 0)
    high, low = two_parts(bwd)
    half = np.concatenate([high, low], 1)
    bwd_op = np.concatenate([half, half], 0)
    l2 = (np.arange(SUB) // EY)[:, None]
    h = (np.arange(LANES) // 64)[None, :]
    cube_plane = plane[None, :]
    zf = np.zeros((2, 2, 2, 2, SUB, LANES))
    zb = np.zeros((2, 2, 2, 2, SUB, LANES))
    rc = np.zeros((2, SUB, LANES))
    for lo in range(2):
        c_out = 2 * (2 * lo + l2) + h
        rc[lo] = rho[c_out]
        for li in range(2):
            for s in range(2):
                for l in range(2):
                    c_in = 2 * (2 * li + (l2 ^ s)) + (h ^ l)
                    zf[lo, l, li, s] = np.roll(der[c_out, c_in] * rho[c_out] * cube_plane, 64 * l, 1)
                    zb[lo, l, li, s] = np.roll(der[c_in, c_out], 64 * l, 1)
    consts = np.concatenate([zf.reshape(-1, SUB, LANES), zb.reshape(-1, SUB, LANES), rc], 0)
    return fwd_op, bwd_op, consts.astype(np.float32)


def roll_sub(x, by):
    return pltpu.roll(x, by % SUB, axis=x.ndim - 2)


def roll_lane(x, by):
    return pltpu.roll(x, by % LANES, axis=x.ndim - 1)


def split(x):
    high = x.astype(jnp.bfloat16)
    return high, (x - high.astype(jnp.float32)).astype(jnp.bfloat16)


def iotas():
    sub = lax.broadcasted_iota(jnp.int32, (SUB, LANES), 0)
    lane = lax.broadcasted_iota(jnp.int32, (SUB, LANES), 1)
    return sub, lane


def lane_gather(x, index):
    return jnp.take_along_axis(x, index, axis=1, mode="promise_in_bounds")


def flip(x, sub, lane):
    y = lane_gather(x, lane ^ 7)
    e = sub % EY
    return jnp.where(
        e == 0, roll_sub(y, -3), jnp.where(e == 1, roll_sub(y, -1), jnp.where(e == 2, roll_sub(y, 1), roll_sub(y, 3)))
    )


def apply_z(pair, consts, base):
    terms = []
    for v in pair:
        terms += [v, roll_sub(v, 4)]
    out = []
    for lo in range(2):
        near, far = (
            sum_of([consts[base + 8 * lo + 4 * half + t] * terms[t] for t in range(4)])
            for half in range(2)
        )
        out.append(near + roll_lane(far, 64))
    return out


def sum_of(parts):
    return (parts[0] + parts[1]) + (parts[2] + parts[3])


def slab_work(sb, u_ref, m_ref, fm_ref, fwd_ref, bwd_ref, consts, put_v, put_faces):
    rows = sb * 64
    u = u_ref[...]
    high, low = split(u)
    g = jnp.dot(
        jnp.concatenate([high, low, high], 1), fwd_ref[...], preferred_element_type=jnp.float32
    )
    m = m_ref[...].reshape(sb * EZ, 3, 16, LANES)
    gx = g[:, :LANES].reshape(sb * EZ, 16, LANES)
    gy = g[:, LANES:].reshape(sb * EZ, 16, LANES)
    fx = (gx * m[:, 0]).reshape(rows, LANES)
    fy = (gy * m[:, 1]).reshape(rows, LANES)
    xh, xl = split(fx)
    yh, yl = split(fy)
    r = jnp.dot(
        jnp.concatenate([xh, yh, xl, yl], 1), bwd_ref[...], preferred_element_type=jnp.float32
    )
    r = (r[:, :LANES] + r[:, LANES:]).reshape(sb * EZ, 2, SUB, LANES)
    u4 = u.reshape(sb * EZ, 2, SUB, LANES)
    mz = m[:, 2].reshape(sb * EZ, 2, SUB, LANES)
    sub, lane = iotas()
    ey, b = sub % EY, lane // 8 % 8
    mask_up = (ey < EY - 1) & (b == 7)
    mask_dn = (ey > 0) & (b == 0)
    top_mask = (sub >= 4) & (lane >= 64)
    bot_mask = (sub < 4) & (lane < 64)
    group = lane // 16 % 4
    pick = (lane % 16) * 8 + 7 * (lane // 64)
    edges = [None, None]
    z_hold = None
    for s in range(sb):
        v = []
        for ez in range(EZ):
            i = s * EZ + ez
            gz = apply_z([u4[i, 0], u4[i, 1]], consts, 0)
            out = apply_z([gz[0] * mz[i, 0], gz[1] * mz[i, 1]], consts, 16)
            for t in range(2):
                w = out[t] + consts[32 + t] * r[i, t]
                up = roll_lane(roll_sub(w, -1), 56)
                dn = roll_lane(roll_sub(w, 1), -56)
                v.append(w + jnp.where(mask_up, up, 0.0) + jnp.where(mask_dn, dn, 0.0))
        for ez in range(EZ - 1):
            a, c = v[2 * ez + 1], v[2 * ez + 2]
            v[2 * ez + 1] = a + jnp.where(top_mask, roll_lane(roll_sub(c, 4), 64), 0.0)
            v[2 * ez + 2] = c + jnp.where(bot_mask, roll_lane(roll_sub(a, 4), 64), 0.0)
        packs = []
        for k in range(8):
            put_v(s, k, v[k])
            got = lane_gather(v[k], pick)
            if k % 4 == 0:
                packs.append(got)
            else:
                packs[-1] = jnp.where(group == k % 4, got, packs[-1])
        low_half = lane < 64
        left = jnp.where(low_half, packs[0], roll_lane(packs[1], 64))
        right = jnp.where(low_half, roll_lane(packs[0], 64), packs[1])
        flag = jnp.broadcast_to(fm_ref[s : s + 1, 0:1], (SUB, LANES)) != 0
        right = jnp.where(flag, flip(right, sub, lane), right)
        put_faces(0, s, right)
        put_faces(1, s, left)
        for side, face in enumerate((right, left)):
            edge = roll_sub(jnp.where(sub < 4, face, roll_lane(face, 8)), 4)
            edge = roll_lane(edge, 8 * s) if s else edge
            edges[side] = edge if s == 0 else jnp.where(lane // 8 == s, edge, edges[side])
        z = jnp.where(sub < 4, v[0], v[7])
        if s % 2 == 0:
            z_hold = z
        else:
            put_faces(2, s // 2, jnp.where((sub < 4) == (lane < 64), z_hold, roll_lane(z, 64)))
    put_faces(3, 0, edges[0])
    put_faces(4, 0, edges[1])


def local_kernel(
    sb, steps, peers, u_ref, m_ref, fm_ref, fwd_ref, bwd_ref, consts,
    v_ref, *refs
):
    landing, sending, (send_sem, recv_sem) = refs[:5], refs[5:10], refs[10:]
    step = pl.program_id(0)
    me, layer = lax.axis_index("slab"), lax.axis_index("layer")
    right, left = lax.rem(me + 1, peers), lax.rem(me + peers - 1, peers)
    targets = (
        {"slab": right, "layer": layer},
        {"slab": left, "layer": layer},
        {"slab": me, "layer": 1 - layer},
        {"slab": right, "layer": 1 - layer},
        {"slab": left, "layer": 1 - layer},
    )
    sizes = (sb, sb, sb // 2, 1, 1)
    barrier = pltpu.get_barrier_semaphore()

    def copy_of(which, at):
        rows = pl.ds(at * sizes[which], sizes[which])
        return pltpu.make_async_remote_copy(
            src_ref=sending[which].at[rows],
            dst_ref=landing[which].at[rows],
            send_sem=send_sem.at[which, at],
            recv_sem=recv_sem.at[which, at],
            device_id=targets[which],
            device_id_type=pl.DeviceIdType.MESH,
        )

    @pl.when(step == 0)
    def _():
        for target in targets:
            pl.semaphore_signal(
                barrier, inc=1, device_id=target, device_id_type=pl.DeviceIdType.MESH
            )

    @pl.when(step == 1)
    def _():
        pl.semaphore_wait(barrier, 5)

    @pl.when(step > 0)
    def _():
        for which in range(5):
            copy_of(which, step - 1).start()

    def put_v(s, k, value):
        v_ref[pl.ds(s * 64 + k * 8, 8), :] = value

    def put_faces(which, at, value):
        sending[which][step * sizes[which] + at] = value

    slab_work(sb, u_ref, m_ref, fm_ref, fwd_ref, bwd_ref, consts, put_v, put_faces)

    @pl.when(step == steps - 1)
    def _():
        def drain(at, carry):
            for which in range(5):
                copy_of(which, at).wait_send()
            return carry

        def collect(at, carry):
            for which in range(5):
                copy_of(which, at).wait_recv()
            return carry

        lax.fori_loop(0, steps - 1, drain, 0)
        for which in range(5):
            copy_of(which, steps - 1).start()
        drain(steps - 1, 0)
        lax.fori_loop(0, steps, collect, 0)


def finish_kernel(
    sb, per_edge, slabs, peers, ids_ref, v_ref, fm_ref, pr_ref, pl_ref, z_ref, er_ref, el_ref, out_ref, inv_ref
):
    step = pl.program_id(0)
    me = lax.axis_index("slab")
    total = slabs * peers
    behind = lax.rem(me + peers - 1, peers) * slabs
    ahead = lax.rem(me + 1, peers) * slabs

    @pl.when(step == 0)
    def _():
        for p in range(slabs):
            inv_ref[0, lax.div(ids_ref[behind + p], peers)] = p
            inv_ref[1, lax.div(ids_ref[ahead + p], peers)] = p

    sub, lane = iotas()
    top_mask = (sub >= 4) & (lane >= 64)
    bot_mask = (sub < 4) & (lane < 64)
    a = lane % 8
    on_face = (a == 0) | (a == 7)
    spread = lane // 8 + 64 * (a == 7).astype(jnp.int32)

    def edge_of(ref, q):
        e = pltpu.roll(ref[lax.div(q, per_edge)], LANES - 8 * lax.rem(q, per_edge), axis=1)
        return jnp.where(
            (sub < 4) & (lane < 8), e, jnp.where((sub >= 4) & (lane >= 120), roll_lane(e, -8), 0.0)
        )

    packs = []
    for s in range(sb):
        own = ids_ref[me * slabs + step * sb + s]
        q_prev = inv_ref[0, lax.div(lax.rem(own + total - 1, total), peers)]
        q_next = inv_ref[1, lax.div(lax.rem(own + 1, total), peers)]
        left = pr_ref[q_prev] + edge_of(er_ref, q_prev)
        right = pl_ref[q_next] + edge_of(el_ref, q_next)
        flag = jnp.broadcast_to(fm_ref[s : s + 1, 0:1], (SUB, LANES)) != 0
        right = jnp.where(flag, flip(right, sub, lane), right)
        z = z_ref[s // 2]
        if s % 2:
            z = roll_lane(z, 64)
        z = roll_lane(roll_sub(z, 4), 64)
        low_half = lane < 64
        packs.append(
            (
                jnp.where(low_half, left, roll_lane(right, 64)),
                jnp.where(low_half, roll_lane(left, 64), right),
                z,
            )
        )
    for k in range(8):
        for s in range(sb):
            w = v_ref[pl.ds(s * 64 + k * 8, 8), :]
            w = w + jnp.where(on_face, lane_gather(packs[s][k // 4], spread + 16 * (k % 4)), 0.0)
            if k == 0:
                w = w + jnp.where(bot_mask, packs[s][2], 0.0)
            if k == 7:
                w = w + jnp.where(top_mask, packs[s][2], 0.0)
            out_ref[pl.ds(s * 64 + k * 8, 8), :] = w


def body(sb, sbf, peers, nodal_field, metric, slab_ids, face_map):
    slabs = nodal_field.shape[1]
    steps = slabs // sb
    fwd_op, bwd_op, consts = tables()
    u = nodal_field.reshape(slabs, EZ, EY, 4, LANES).transpose(0, 1, 3, 2, 4).reshape(slabs * 64, LANES)
    m = (
        metric.reshape(slabs, EZ, EY, 3, 4, LANES)
        .transpose(0, 1, 3, 4, 2, 5)
        .reshape(slabs * 192, LANES)
    )
    f32 = jnp.float32
    whole = lambda shape: pl.BlockSpec(shape, lambda i: (0,) * len(shape))
    stack = lambda n: pl.BlockSpec((n, SUB, LANES), lambda i: (i, 0, 0))
    v, pr, plf, z, er, el = pl.pallas_call(
        functools.partial(local_kernel, sb, steps, peers),
        grid=(steps,),
        in_specs=[
            pl.BlockSpec((sb * 64, LANES), lambda i: (i, 0)),
            pl.BlockSpec((sb * 192, LANES), lambda i: (i, 0)),
            pl.BlockSpec((sb, LANES), lambda i: (i, 0)),
            whole(fwd_op.shape),
            whole(bwd_op.shape),
            whole(consts.shape),
        ],
        out_specs=[
            pl.BlockSpec((sb * 64, LANES), lambda i: (i, 0)),
            *[pl.BlockSpec(memory_space=pl.ANY)] * 5,
        ],
        out_shape=[
            jax.ShapeDtypeStruct((slabs * 64, LANES), f32),
            jax.ShapeDtypeStruct((slabs, SUB, LANES), f32),
            jax.ShapeDtypeStruct((slabs, SUB, LANES), f32),
            jax.ShapeDtypeStruct((slabs // 2, SUB, LANES), f32),
            jax.ShapeDtypeStruct((steps, SUB, LANES), f32),
            jax.ShapeDtypeStruct((steps, SUB, LANES), f32),
        ],
        scratch_shapes=[
            pltpu.VMEM((slabs, SUB, LANES), f32),
            pltpu.VMEM((slabs, SUB, LANES), f32),
            pltpu.VMEM((slabs // 2, SUB, LANES), f32),
            pltpu.VMEM((steps, SUB, LANES), f32),
            pltpu.VMEM((steps, SUB, LANES), f32),
            pltpu.SemaphoreType.DMA((5, steps)),
            pltpu.SemaphoreType.DMA((5, steps)),
        ],
        compiler_params=pltpu.CompilerParams(collective_id=0, has_side_effects=True),
        name="local",
    )(u, m, face_map, jnp.asarray(fwd_op), jnp.asarray(bwd_op), jnp.asarray(consts))
    out = pl.pallas_call(
        functools.partial(finish_kernel, sbf, sb, slabs, peers),
        grid=(slabs // sbf,),
        in_specs=[
            pl.BlockSpec(memory_space=pltpu.SMEM),
            pl.BlockSpec((sbf * 64, LANES), lambda i: (i, 0)),
            pl.BlockSpec((sbf, LANES), lambda i: (i, 0)),
            whole((slabs, SUB, LANES)),
            whole((slabs, SUB, LANES)),
            stack(sbf // 2),
            whole((steps, SUB, LANES)),
            whole((steps, SUB, LANES)),
        ],
        out_specs=pl.BlockSpec((sbf * 64, LANES), lambda i: (i, 0)),
        out_shape=jax.ShapeDtypeStruct((slabs * 64, LANES), f32),
        scratch_shapes=[pltpu.SMEM((2, slabs), jnp.int32)],
        name="finish",
    )(slab_ids, v, face_map, pr, plf, z, er, el)
    out = out.reshape(slabs, EZ, 4, EY, LANES).transpose(0, 1, 3, 2, 4)
    return out.reshape(1, slabs, EZ, EY, PTS)


def solution(mesh):
    return jax.shard_map(
        functools.partial(body, SB, SBF, mesh.shape["slab"]),
        mesh=mesh,
        in_specs=(
            P("layer", "slab", None, None, None),
            P("layer", "slab", None, None, None, None),
            P(),
            P("slab", None),
        ),
        out_specs=P("layer", "slab", None, None, None),
        check_vma=False,
    )
```

```python
import functools

import jax
import jax.numpy as jnp
import numpy as np
from jax import lax
from jax.experimental import pallas as pl
from jax.experimental.pallas import tpu as pltpu
from jax.sharding import PartitionSpec as P

P_SIZE = 8
PTS = 512
EY = 4
EZ = 4
SUB = 8
LANES = 128
CHUNK = 4
SB = 8
FLAGS = None
SBF = 8


def legendre_pair(nodes, degree):
    lower = nodes * 0.0 + 1.0
    upper = nodes.copy()
    for order in range(2, degree + 1):
        lower, upper = upper, ((2 * order - 1) * nodes * upper - (order - 1) * lower) / order
    return lower, upper


def gll_tables():
    degree = P_SIZE - 1
    nodes = -np.cos(np.pi * np.arange(P_SIZE) / degree)
    for _ in range(100):
        lower, upper = legendre_pair(nodes, degree)
        nodes = nodes - (nodes * upper - lower) / ((degree + 1) * upper)
    lower, upper = legendre_pair(nodes, degree)
    rho = 2.0 / (degree * (degree + 1) * upper * upper)
    eye = np.eye(P_SIZE)
    differ = nodes[:, None] - nodes[None, :] + eye
    der = upper[:, None] / (upper[None, :] * differ) * (1.0 - eye)
    der[0, 0] = -degree * (degree + 1) / 4.0
    der[degree, degree] = degree * (degree + 1) / 4.0
    return der, rho


def two_parts(table):
    high = np.asarray(table, np.float32).astype(jnp.bfloat16)
    low = (table - high.astype(np.float64)).astype(jnp.bfloat16)
    return high, low


def tables():
    der, rho = gll_tables()
    eye8, eye2 = np.eye(8), np.eye(2)
    plane = np.tile(np.kron(rho, rho), 2)
    fwd = np.concatenate(
        [np.kron(np.eye(16), der.T) * plane, np.kron(eye2, np.kron(der.T, eye8)) * plane], 1
    )
    high, low = two_parts(fwd)
    fwd_op = np.concatenate([high, high, low], 0)
    bwd = np.concatenate([np.kron(np.eye(16), der), np.kron(eye2, np.kron(der, eye8))], 0)
    high, low = two_parts(bwd)
    half = np.concatenate([high, low], 1)
    bwd_op = np.concatenate([half, half], 0)
    l2 = (np.arange(SUB) // EY)[:, None]
    h = (np.arange(LANES) // 64)[None, :]
    cube_plane = plane[None, :]
    zf = np.zeros((2, 2, 2, 2, SUB, LANES))
    zb = np.zeros((2, 2, 2, 2, SUB, LANES))
    rc = np.zeros((2, SUB, LANES))
    for lo in range(2):
        c_out = 2 * (2 * lo + l2) + h
        rc[lo] = rho[c_out]
        for li in range(2):
            for s in range(2):
                for l in range(2):
                    c_in = 2 * (2 * li + (l2 ^ s)) + (h ^ l)
                    zf[lo, l, li, s] = np.roll(der[c_out, c_in] * rho[c_out] * cube_plane, 64 * l, 1)
                    zb[lo, l, li, s] = np.roll(der[c_in, c_out], 64 * l, 1)
    consts = np.concatenate([zf.reshape(-1, SUB, LANES), zb.reshape(-1, SUB, LANES), rc], 0)
    return fwd_op, bwd_op, consts.astype(np.float32)


def roll_sub(x, by):
    return pltpu.roll(x, by % SUB, axis=x.ndim - 2)


def roll_lane(x, by):
    return pltpu.roll(x, by % LANES, axis=x.ndim - 1)


def split(x):
    high = x.astype(jnp.bfloat16)
    return high, (x - high.astype(jnp.float32)).astype(jnp.bfloat16)


def iotas():
    sub = lax.broadcasted_iota(jnp.int32, (SUB, LANES), 0)
    lane = lax.broadcasted_iota(jnp.int32, (SUB, LANES), 1)
    return sub, lane


def lane_gather(x, index):
    return jnp.take_along_axis(x, index, axis=1, mode="promise_in_bounds")


def flip(x, sub, lane):
    y = lane_gather(x, lane ^ 7)
    e = sub % EY
    return jnp.where(
        e == 0, roll_sub(y, -3), jnp.where(e == 1, roll_sub(y, -1), jnp.where(e == 2, roll_sub(y, 1), roll_sub(y, 3)))
    )


def apply_z(pair, consts, base):
    terms = []
    for v in pair:
        terms += [v, roll_sub(v, 4)]
    out = []
    for lo in range(2):
        near, far = (
            sum_of([consts[base + 8 * lo + 4 * half + t] * terms[t] for t in range(4)])
            for half in range(2)
        )
        out.append(near + roll_lane(far, 64))
    return out


def sum_of(parts):
    return (parts[0] + parts[1]) + (parts[2] + parts[3])


def slab_work(sb, u_ref, m_ref, fm_ref, fwd_ref, bwd_ref, consts, put_v, put_faces):
    edges = [None, None]
    for first in range(0, sb, CHUNK):
        chunk_work(
            first, CHUNK, u_ref, m_ref, fm_ref, fwd_ref, bwd_ref, consts, put_v, put_faces, edges
        )
    put_faces(3, 0, edges[0])
    put_faces(4, 0, edges[1])


def chunk_work(
    first, sb, u_ref, m_ref, fm_ref, fwd_ref, bwd_ref, consts, put_v, put_faces, edges
):
    rows = sb * 64
    u = u_ref[pl.ds(first * 64, rows), :]
    high, low = split(u)
    g = jnp.dot(
        jnp.concatenate([high, low, high], 1), fwd_ref[...], preferred_element_type=jnp.float32
    )
    m = m_ref[pl.ds(first * 192, sb * 192), :].reshape(sb * EZ, 3, 16, LANES)
    gx = g[:, :LANES].reshape(sb * EZ, 16, LANES)
    gy = g[:, LANES:].reshape(sb * EZ, 16, LANES)
    fx = (gx * m[:, 0]).reshape(rows, LANES)
    fy = (gy * m[:, 1]).reshape(rows, LANES)
    xh, xl = split(fx)
    yh, yl = split(fy)
    r = jnp.dot(
        jnp.concatenate([xh, yh, xl, yl], 1), bwd_ref[...], preferred_element_type=jnp.float32
    )
    r = (r[:, :LANES] + r[:, LANES:]).reshape(sb * EZ, 2, SUB, LANES)
    u4 = u.reshape(sb * EZ, 2, SUB, LANES)
    mz = m[:, 2].reshape(sb * EZ, 2, SUB, LANES)
    sub, lane = iotas()
    ey, b = sub % EY, lane // 8 % 8
    mask_up = (ey < EY - 1) & (b == 7)
    mask_dn = (ey > 0) & (b == 0)
    top_mask = (sub >= 4) & (lane >= 64)
    bot_mask = (sub < 4) & (lane < 64)
    group = lane // 16 % 4
    pick = (lane % 16) * 8 + 7 * (lane // 64)
    z_hold = None
    for j in range(sb):
        s = first + j
        v = []
        for ez in range(EZ):
            i = j * EZ + ez
            gz = apply_z([u4[i, 0], u4[i, 1]], consts, 0)
            out = apply_z([gz[0] * mz[i, 0], gz[1] * mz[i, 1]], consts, 16)
            for t in range(2):
                w = out[t] + consts[32 + t] * r[i, t]
                up = roll_lane(roll_sub(w, -1), 56)
                dn = roll_lane(roll_sub(w, 1), -56)
                v.append(w + jnp.where(mask_up, up, 0.0) + jnp.where(mask_dn, dn, 0.0))
        for ez in range(EZ - 1):
            a, c = v[2 * ez + 1], v[2 * ez + 2]
            v[2 * ez + 1] = a + jnp.where(top_mask, roll_lane(roll_sub(c, 4), 64), 0.0)
            v[2 * ez + 2] = c + jnp.where(bot_mask, roll_lane(roll_sub(a, 4), 64), 0.0)
        packs = []
        for k in range(8):
            put_v(s, k, v[k])
            got = lane_gather(v[k], pick)
            if k % 4 == 0:
                packs.append(got)
            else:
                packs[-1] = jnp.where(group == k % 4, got, packs[-1])
        low_half = lane < 64
        left = jnp.where(low_half, packs[0], roll_lane(packs[1], 64))
        right = jnp.where(low_half, roll_lane(packs[0], 64), packs[1])
        flag = jnp.broadcast_to(fm_ref[s : s + 1, 0:1], (SUB, LANES)) != 0
        right = jnp.where(flag, flip(right, sub, lane), right)
        put_faces(0, s, right)
        put_faces(1, s, left)
        for side, face in enumerate((right, left)):
            edge = roll_sub(jnp.where(sub < 4, face, roll_lane(face, 8)), 4)
            edge = roll_lane(edge, 8 * s) if s else edge
            edges[side] = edge if s == 0 else jnp.where(lane // 8 == s, edge, edges[side])
        z = jnp.where(sub < 4, v[0], v[7])
        if s % 2 == 0:
            z_hold = z
        else:
            put_faces(2, s // 2, jnp.where((sub < 4) == (lane < 64), z_hold, roll_lane(z, 64)))


def local_kernel(
    sb, steps, peers, u_ref, m_ref, fm_ref, fwd_ref, bwd_ref, consts,
    v_ref, *refs
):
    landing, sending, (send_sem, recv_sem) = refs[:5], refs[5:10], refs[10:]
    step = pl.program_id(0)
    me, layer = lax.axis_index("slab"), lax.axis_index("layer")
    right, left = lax.rem(me + 1, peers), lax.rem(me + peers - 1, peers)
    targets = (
        {"slab": right, "layer": layer},
        {"slab": left, "layer": layer},
        {"slab": me, "layer": 1 - layer},
        {"slab": right, "layer": 1 - layer},
        {"slab": left, "layer": 1 - layer},
    )
    sizes = (sb, sb, sb // 2, 1, 1)
    barrier = pltpu.get_barrier_semaphore()

    def copy_of(which, at):
        rows = pl.ds(at * sizes[which], sizes[which])
        return pltpu.make_async_remote_copy(
            src_ref=sending[which].at[rows],
            dst_ref=landing[which].at[rows],
            send_sem=send_sem.at[which, at],
            recv_sem=recv_sem.at[which, at],
            device_id=targets[which],
            device_id_type=pl.DeviceIdType.MESH,
        )

    @pl.when(step == 0)
    def _():
        for target in targets:
            pl.semaphore_signal(
                barrier, inc=1, device_id=target, device_id_type=pl.DeviceIdType.MESH
            )

    @pl.when(step == 1)
    def _():
        pl.semaphore_wait(barrier, 5)

    @pl.when(step > 0)
    def _():
        for which in range(5):
            copy_of(which, step - 1).start()

    def put_v(s, k, value):
        v_ref[pl.ds(s * 64 + k * 8, 8), :] = value

    def put_faces(which, at, value):
        sending[which][step * sizes[which] + at] = value

    slab_work(sb, u_ref, m_ref, fm_ref, fwd_ref, bwd_ref, consts, put_v, put_faces)

    @pl.when(step == steps - 1)
    def _():
        def drain(at, carry):
            for which in range(5):
                copy_of(which, at).wait_send()
            return carry

        def collect(at, carry):
            for which in range(5):
                copy_of(which, at).wait_recv()
            return carry

        lax.fori_loop(0, steps - 1, drain, 0)
        for which in range(5):
            copy_of(which, steps - 1).start()
        drain(steps - 1, 0)
        lax.fori_loop(0, steps, collect, 0)


def finish_kernel(
    sb, per_edge, slabs, peers, ids_ref, v_ref, fm_ref, pr_ref, pl_ref, z_ref, er_ref, el_ref, out_ref, inv_ref
):
    step = pl.program_id(0)
    me = lax.axis_index("slab")
    total = slabs * peers
    behind = lax.rem(me + peers - 1, peers) * slabs
    ahead = lax.rem(me + 1, peers) * slabs

    @pl.when(step == 0)
    def _():
        for p in range(slabs):
            inv_ref[0, lax.div(ids_ref[behind + p], peers)] = p
            inv_ref[1, lax.div(ids_ref[ahead + p], peers)] = p

    sub, lane = iotas()
    top_mask = (sub >= 4) & (lane >= 64)
    bot_mask = (sub < 4) & (lane < 64)
    a = lane % 8
    on_face = (a == 0) | (a == 7)
    spread = lane // 8 + 64 * (a == 7).astype(jnp.int32)

    def edge_of(ref, q):
        e = pltpu.roll(ref[lax.div(q, per_edge)], LANES - 8 * lax.rem(q, per_edge), axis=1)
        return jnp.where(
            (sub < 4) & (lane < 8), e, jnp.where((sub >= 4) & (lane >= 120), roll_lane(e, -8), 0.0)
        )

    packs = []
    for s in range(sb):
        own = ids_ref[me * slabs + step * sb + s]
        q_prev = inv_ref[0, lax.div(lax.rem(own + total - 1, total), peers)]
        q_next = inv_ref[1, lax.div(lax.rem(own + 1, total), peers)]
        left = pr_ref[q_prev] + edge_of(er_ref, q_prev)
        right = pl_ref[q_next] + edge_of(el_ref, q_next)
        flag = jnp.broadcast_to(fm_ref[s : s + 1, 0:1], (SUB, LANES)) != 0
        right = jnp.where(flag, flip(right, sub, lane), right)
        z = z_ref[s // 2]
        if s % 2:
            z = roll_lane(z, 64)
        z = roll_lane(roll_sub(z, 4), 64)
        low_half = lane < 64
        packs.append(
            (
                jnp.where(low_half, left, roll_lane(right, 64)),
                jnp.where(low_half, roll_lane(left, 64), right),
                z,
            )
        )
    for k in range(8):
        for s in range(sb):
            w = v_ref[pl.ds(s * 64 + k * 8, 8), :]
            w = w + jnp.where(on_face, lane_gather(packs[s][k // 4], spread + 16 * (k % 4)), 0.0)
            if k == 0:
                w = w + jnp.where(bot_mask, packs[s][2], 0.0)
            if k == 7:
                w = w + jnp.where(top_mask, packs[s][2], 0.0)
            out_ref[pl.ds(s * 64 + k * 8, 8), :] = w


def body(sb, sbf, peers, nodal_field, metric, slab_ids, face_map):
    slabs = nodal_field.shape[1]
    steps = slabs // sb
    fwd_op, bwd_op, consts = tables()
    u = nodal_field.reshape(slabs, EZ, EY, 4, LANES).transpose(0, 1, 3, 2, 4).reshape(slabs * 64, LANES)
    m = (
        metric.reshape(slabs, EZ, EY, 3, 4, LANES)
        .transpose(0, 1, 3, 4, 2, 5)
        .reshape(slabs * 192, LANES)
    )
    f32 = jnp.float32
    whole = lambda shape: pl.BlockSpec(shape, lambda i: (0,) * len(shape))
    stack = lambda n: pl.BlockSpec((n, SUB, LANES), lambda i: (i, 0, 0))
    v, pr, plf, z, er, el = pl.pallas_call(
        functools.partial(local_kernel, sb, steps, peers),
        grid=(steps,),
        in_specs=[
            pl.BlockSpec((sb * 64, LANES), lambda i: (i, 0)),
            pl.BlockSpec((sb * 192, LANES), lambda i: (i, 0)),
            pl.BlockSpec((sb, LANES), lambda i: (i, 0)),
            whole(fwd_op.shape),
            whole(bwd_op.shape),
            whole(consts.shape),
        ],
        out_specs=[
            pl.BlockSpec((sb * 64, LANES), lambda i: (i, 0)),
            *[pl.BlockSpec(memory_space=pl.ANY)] * 5,
        ],
        out_shape=[
            jax.ShapeDtypeStruct((slabs * 64, LANES), f32),
            jax.ShapeDtypeStruct((slabs, SUB, LANES), f32),
            jax.ShapeDtypeStruct((slabs, SUB, LANES), f32),
            jax.ShapeDtypeStruct((slabs // 2, SUB, LANES), f32),
            jax.ShapeDtypeStruct((steps, SUB, LANES), f32),
            jax.ShapeDtypeStruct((steps, SUB, LANES), f32),
        ],
        scratch_shapes=[
            pltpu.VMEM((slabs, SUB, LANES), f32),
            pltpu.VMEM((slabs, SUB, LANES), f32),
            pltpu.VMEM((slabs // 2, SUB, LANES), f32),
            pltpu.VMEM((steps, SUB, LANES), f32),
            pltpu.VMEM((steps, SUB, LANES), f32),
            pltpu.SemaphoreType.DMA((5, steps)),
            pltpu.SemaphoreType.DMA((5, steps)),
        ],
        compiler_params=pltpu.CompilerParams(
            collective_id=0, has_side_effects=True, flags=FLAGS
        ),
        name="local",
    )(u, m, face_map, jnp.asarray(fwd_op), jnp.asarray(bwd_op), jnp.asarray(consts))
    out = pl.pallas_call(
        functools.partial(finish_kernel, sbf, sb, slabs, peers),
        grid=(slabs // sbf,),
        in_specs=[
            pl.BlockSpec(memory_space=pltpu.SMEM),
            pl.BlockSpec((sbf * 64, LANES), lambda i: (i, 0)),
            pl.BlockSpec((sbf, LANES), lambda i: (i, 0)),
            whole((slabs, SUB, LANES)),
            whole((slabs, SUB, LANES)),
            stack(sbf // 2),
            whole((steps, SUB, LANES)),
            whole((steps, SUB, LANES)),
        ],
        out_specs=pl.BlockSpec((sbf * 64, LANES), lambda i: (i, 0)),
        out_shape=jax.ShapeDtypeStruct((slabs * 64, LANES), f32),
        scratch_shapes=[pltpu.SMEM((2, slabs), jnp.int32)],
        name="finish",
    )(slab_ids, v, face_map, pr, plf, z, er, el)
    out = out.reshape(slabs, EZ, 4, EY, LANES).transpose(0, 1, 3, 2, 4)
    return out.reshape(1, slabs, EZ, EY, PTS)


def solution(mesh):
    return jax.shard_map(
        functools.partial(body, SB, SBF, mesh.shape["slab"]),
        mesh=mesh,
        in_specs=(
            P("layer", "slab", None, None, None),
            P("layer", "slab", None, None, None, None),
            P(),
            P("slab", None),
        ),
        out_specs=P("layer", "slab", None, None, None),
        check_vma=False,
    )
```

```python
import functools

import jax
import jax.numpy as jnp
import numpy as np
from jax import lax
from jax.experimental import pallas as pl
from jax.experimental.pallas import tpu as pltpu
from jax.sharding import PartitionSpec as P

P_SIZE = 8
PTS = 512
EY = 4
EZ = 4
SUB = 8
LANES = 128
SB = 8
SBF = 16


def legendre_pair(nodes, degree):
    lower = nodes * 0.0 + 1.0
    upper = nodes.copy()
    for order in range(2, degree + 1):
        lower, upper = upper, ((2 * order - 1) * nodes * upper - (order - 1) * lower) / order
    return lower, upper


def gll_tables():
    degree = P_SIZE - 1
    nodes = -np.cos(np.pi * np.arange(P_SIZE) / degree)
    for _ in range(100):
        lower, upper = legendre_pair(nodes, degree)
        nodes = nodes - (nodes * upper - lower) / ((degree + 1) * upper)
    lower, upper = legendre_pair(nodes, degree)
    rho = 2.0 / (degree * (degree + 1) * upper * upper)
    eye = np.eye(P_SIZE)
    differ = nodes[:, None] - nodes[None, :] + eye
    der = upper[:, None] / (upper[None, :] * differ) * (1.0 - eye)
    der[0, 0] = -degree * (degree + 1) / 4.0
    der[degree, degree] = degree * (degree + 1) / 4.0
    return der, rho


def two_parts(table):
    high = np.asarray(table, np.float32).astype(jnp.bfloat16)
    low = (table - high.astype(np.float64)).astype(jnp.bfloat16)
    return high, low


def tables():
    der, rho = gll_tables()
    eye8, eye2 = np.eye(8), np.eye(2)
    plane = np.tile(np.kron(rho, rho), 2)
    fwd = np.concatenate(
        [np.kron(np.eye(16), der.T) * plane, np.kron(eye2, np.kron(der.T, eye8)) * plane], 1
    )
    high, low = two_parts(fwd)
    fwd_op = np.concatenate([high, high, low], 0)
    bwd = np.concatenate([np.kron(np.eye(16), der), np.kron(eye2, np.kron(der, eye8))], 0)
    high, low = two_parts(bwd)
    half = np.concatenate([high, low], 1)
    bwd_op = np.concatenate([half, half], 0)
    l2 = (np.arange(SUB) // EY)[:, None]
    h = (np.arange(LANES) // 64)[None, :]
    cube_plane = plane[None, :]
    zf = np.zeros((2, 2, 2, 2, SUB, LANES))
    zb = np.zeros((2, 2, 2, 2, SUB, LANES))
    rc = np.zeros((2, SUB, LANES))
    for lo in range(2):
        c_out = 2 * (2 * lo + l2) + h
        rc[lo] = rho[c_out]
        for li in range(2):
            for s in range(2):
                for l in range(2):
                    c_in = 2 * (2 * li + (l2 ^ s)) + (h ^ l)
                    zf[lo, l, li, s] = np.roll(der[c_out, c_in] * rho[c_out] * cube_plane, 64 * l, 1)
                    zb[lo, l, li, s] = np.roll(der[c_in, c_out], 64 * l, 1)
    consts = np.concatenate([zf.reshape(-1, SUB, LANES), zb.reshape(-1, SUB, LANES), rc], 0)
    return fwd_op, bwd_op, consts.astype(np.float32)


def roll_sub(x, by):
    return pltpu.roll(x, by % SUB, axis=x.ndim - 2)


def roll_lane(x, by):
    return pltpu.roll(x, by % LANES, axis=x.ndim - 1)


def split(x):
    high = x.astype(jnp.bfloat16)
    return high, (x - high.astype(jnp.float32)).astype(jnp.bfloat16)


def iotas():
    sub = lax.broadcasted_iota(jnp.int32, (SUB, LANES), 0)
    lane = lax.broadcasted_iota(jnp.int32, (SUB, LANES), 1)
    return sub, lane


def lane_gather(x, index):
    return jnp.take_along_axis(x, index, axis=1, mode="promise_in_bounds")


def flip(x, sub, lane):
    y = lane_gather(x, lane ^ 7)
    e = sub % EY
    return jnp.where(
        e == 0, roll_sub(y, -3), jnp.where(e == 1, roll_sub(y, -1), jnp.where(e == 2, roll_sub(y, 1), roll_sub(y, 3)))
    )


def apply_z(pair, consts, base):
    terms = []
    for v in pair:
        terms += [v, roll_sub(v, 4)]
    out = []
    for lo in range(2):
        near, far = (
            sum_of([consts[base + 8 * lo + 4 * half + t] * terms[t] for t in range(4)])
            for half in range(2)
        )
        out.append(near + roll_lane(far, 64))
    return out


def sum_of(parts):
    return (parts[0] + parts[1]) + (parts[2] + parts[3])


def slab_work(sb, u_ref, m_ref, fm_ref, fwd_ref, bwd_ref, consts, put_v, put_faces):
    rows = sb * 64
    u = u_ref[...]
    high, low = split(u)
    g = jnp.dot(
        jnp.concatenate([high, low, high], 1), fwd_ref[...], preferred_element_type=jnp.float32
    )
    m = m_ref[...].reshape(sb * EZ, 3, 16, LANES)
    gx = g[:, :LANES].reshape(sb * EZ, 16, LANES)
    gy = g[:, LANES:].reshape(sb * EZ, 16, LANES)
    fx = (gx * m[:, 0]).reshape(rows, LANES)
    fy = (gy * m[:, 1]).reshape(rows, LANES)
    xh, xl = split(fx)
    yh, yl = split(fy)
    r = jnp.dot(
        jnp.concatenate([xh, yh, xl, yl], 1), bwd_ref[...], preferred_element_type=jnp.float32
    )
    r = (r[:, :LANES] + r[:, LANES:]).reshape(sb * EZ, 2, SUB, LANES)
    u4 = u.reshape(sb * EZ, 2, SUB, LANES)
    mz = m[:, 2].reshape(sb * EZ, 2, SUB, LANES)
    sub, lane = iotas()
    ey, b = sub % EY, lane // 8 % 8
    mask_up = (ey < EY - 1) & (b == 7)
    mask_dn = (ey > 0) & (b == 0)
    top_mask = (sub >= 4) & (lane >= 64)
    bot_mask = (sub < 4) & (lane < 64)
    group = lane // 16 % 4
    pick = (lane % 16) * 8 + 7 * (lane // 64)
    edges = [None, None]
    z_hold = None
    for s in range(sb):
        v = []
        for ez in range(EZ):
            i = s * EZ + ez
            gz = apply_z([u4[i, 0], u4[i, 1]], consts, 0)
            out = apply_z([gz[0] * mz[i, 0], gz[1] * mz[i, 1]], consts, 16)
            for t in range(2):
                w = out[t] + consts[32 + t] * r[i, t]
                up = roll_lane(roll_sub(w, -1), 56)
                dn = roll_lane(roll_sub(w, 1), -56)
                v.append(w + jnp.where(mask_up, up, 0.0) + jnp.where(mask_dn, dn, 0.0))
        for ez in range(EZ - 1):
            a, c = v[2 * ez + 1], v[2 * ez + 2]
            v[2 * ez + 1] = a + jnp.where(top_mask, roll_lane(roll_sub(c, 4), 64), 0.0)
            v[2 * ez + 2] = c + jnp.where(bot_mask, roll_lane(roll_sub(a, 4), 64), 0.0)
        packs = []
        for k in range(8):
            put_v(s, k, v[k])
            got = lane_gather(v[k], pick)
            if k % 4 == 0:
                packs.append(got)
            else:
                packs[-1] = jnp.where(group == k % 4, got, packs[-1])
        low_half = lane < 64
        left = jnp.where(low_half, packs[0], roll_lane(packs[1], 64))
        right = jnp.where(low_half, roll_lane(packs[0], 64), packs[1])
        flag = jnp.broadcast_to(fm_ref[s : s + 1, 0:1], (SUB, LANES)) != 0
        right = jnp.where(flag, flip(right, sub, lane), right)
        put_faces(0, s, right)
        put_faces(1, s, left)
        for side, face in enumerate((right, left)):
            edge = roll_sub(jnp.where(sub < 4, face, roll_lane(face, 8)), 4)
            edge = roll_lane(edge, 8 * s) if s else edge
            edges[side] = edge if s == 0 else jnp.where(lane // 8 == s, edge, edges[side])
        z = jnp.where(sub < 4, v[0], v[7])
        if s % 2 == 0:
            z_hold = z
        else:
            put_faces(2, s // 2, jnp.where((sub < 4) == (lane < 64), z_hold, roll_lane(z, 64)))
    put_faces(3, 0, edges[0])
    put_faces(4, 0, edges[1])


def local_kernel(
    sb, steps, peers, u_ref, m_ref, fm_ref, fwd_ref, bwd_ref, consts,
    v_ref, *refs
):
    landing, sending, (send_sem, recv_sem) = refs[:5], refs[5:10], refs[10:]
    step = pl.program_id(0)
    me, layer = lax.axis_index("slab"), lax.axis_index("layer")
    right, left = lax.rem(me + 1, peers), lax.rem(me + peers - 1, peers)
    targets = (
        {"slab": right, "layer": layer},
        {"slab": left, "layer": layer},
        {"slab": me, "layer": 1 - layer},
        {"slab": right, "layer": 1 - layer},
        {"slab": left, "layer": 1 - layer},
    )
    sizes = (sb, sb, sb // 2, 1, 1)
    barrier = pltpu.get_barrier_semaphore()

    def copy_of(which, at):
        rows = pl.ds(at * sizes[which], sizes[which])
        return pltpu.make_async_remote_copy(
            src_ref=sending[which].at[rows],
            dst_ref=landing[which].at[rows],
            send_sem=send_sem.at[which, at],
            recv_sem=recv_sem.at[which, at],
            device_id=targets[which],
            device_id_type=pl.DeviceIdType.MESH,
        )

    @pl.when(step == 0)
    def _():
        for target in targets:
            pl.semaphore_signal(
                barrier, inc=1, device_id=target, device_id_type=pl.DeviceIdType.MESH
            )

    @pl.when(step == 1)
    def _():
        pl.semaphore_wait(barrier, 5)

    @pl.when(step > 0)
    def _():
        for which in range(5):
            copy_of(which, step - 1).start()

    def put_v(s, k, value):
        v_ref[pl.ds(s * 64 + k * 8, 8), :] = value

    def put_faces(which, at, value):
        sending[which][step * sizes[which] + at] = value

    slab_work(sb, u_ref, m_ref, fm_ref, fwd_ref, bwd_ref, consts, put_v, put_faces)

    @pl.when(step == steps - 1)
    def _():
        def drain(at, carry):
            for which in range(5):
                copy_of(which, at).wait_send()
            return carry

        def collect(at, carry):
            for which in range(5):
                copy_of(which, at).wait_recv()
            return carry

        lax.fori_loop(0, steps - 2, drain, 0)
        for which in range(5):
            copy_of(which, steps - 1).start()
        drain(steps - 2, 0)
        drain(steps - 1, 0)
        lax.fori_loop(0, steps, collect, 0)


def finish_kernel(
    sb, per_edge, slabs, peers, ids_ref, v_ref, fm_ref, pr_ref, pl_ref, z_ref, er_ref, el_ref, out_ref, inv_ref
):
    step = pl.program_id(0)
    me = lax.axis_index("slab")
    total = slabs * peers
    behind = lax.rem(me + peers - 1, peers) * slabs
    ahead = lax.rem(me + 1, peers) * slabs

    @pl.when(step == 0)
    def _():
        for p in range(slabs):
            inv_ref[0, lax.div(ids_ref[behind + p], peers)] = p
            inv_ref[1, lax.div(ids_ref[ahead + p], peers)] = p

    sub, lane = iotas()
    top_mask = (sub >= 4) & (lane >= 64)
    bot_mask = (sub < 4) & (lane < 64)
    a = lane % 8
    on_face = (a == 0) | (a == 7)
    spread = lane // 8 + 64 * (a == 7).astype(jnp.int32)

    def edge_of(ref, q):
        e = pltpu.roll(ref[lax.div(q, per_edge)], LANES - 8 * lax.rem(q, per_edge), axis=1)
        return jnp.where(
            (sub < 4) & (lane < 8), e, jnp.where((sub >= 4) & (lane >= 120), roll_lane(e, -8), 0.0)
        )

    packs = []
    for s in range(sb):
        own = ids_ref[me * slabs + step * sb + s]
        q_prev = inv_ref[0, lax.div(lax.rem(own + total - 1, total), peers)]
        q_next = inv_ref[1, lax.div(lax.rem(own + 1, total), peers)]
        left = pr_ref[q_prev] + edge_of(er_ref, q_prev)
        right = pl_ref[q_next] + edge_of(el_ref, q_next)
        flag = jnp.broadcast_to(fm_ref[s : s + 1, 0:1], (SUB, LANES)) != 0
        right = jnp.where(flag, flip(right, sub, lane), right)
        z = z_ref[s // 2]
        if s % 2:
            z = roll_lane(z, 64)
        z = roll_lane(roll_sub(z, 4), 64)
        low_half = lane < 64
        packs.append(
            (
                jnp.where(low_half, left, roll_lane(right, 64)),
                jnp.where(low_half, roll_lane(left, 64), right),
                z,
            )
        )
    for k in range(8):
        for s in range(sb):
            w = v_ref[pl.ds(s * 64 + k * 8, 8), :]
            w = w + jnp.where(on_face, lane_gather(packs[s][k // 4], spread + 16 * (k % 4)), 0.0)
            if k == 0:
                w = w + jnp.where(bot_mask, packs[s][2], 0.0)
            if k == 7:
                w = w + jnp.where(top_mask, packs[s][2], 0.0)
            out_ref[pl.ds(s * 64 + k * 8, 8), :] = w


def body(sb, sbf, peers, nodal_field, metric, slab_ids, face_map):
    slabs = nodal_field.shape[1]
    steps = slabs // sb
    fwd_op, bwd_op, consts = tables()
    u = nodal_field.reshape(slabs, EZ, EY, 4, LANES).transpose(0, 1, 3, 2, 4).reshape(slabs * 64, LANES)
    m = (
        metric.reshape(slabs, EZ, EY, 3, 4, LANES)
        .transpose(0, 1, 3, 4, 2, 5)
        .reshape(slabs * 192, LANES)
    )
    f32 = jnp.float32
    whole = lambda shape: pl.BlockSpec(shape, lambda i: (0,) * len(shape))
    stack = lambda n: pl.BlockSpec((n, SUB, LANES), lambda i: (i, 0, 0))
    v, pr, plf, z, er, el = pl.pallas_call(
        functools.partial(local_kernel, sb, steps, peers),
        grid=(steps,),
        in_specs=[
            pl.BlockSpec((sb * 64, LANES), lambda i: (i, 0)),
            pl.BlockSpec((sb * 192, LANES), lambda i: (i, 0)),
            pl.BlockSpec((sb, LANES), lambda i: (i, 0)),
            whole(fwd_op.shape),
            whole(bwd_op.shape),
            whole(consts.shape),
        ],
        out_specs=[
            pl.BlockSpec((sb * 64, LANES), lambda i: (i, 0)),
            *[pl.BlockSpec(memory_space=pl.ANY)] * 5,
        ],
        out_shape=[
            jax.ShapeDtypeStruct((slabs * 64, LANES), f32),
            jax.ShapeDtypeStruct((slabs, SUB, LANES), f32),
            jax.ShapeDtypeStruct((slabs, SUB, LANES), f32),
            jax.ShapeDtypeStruct((slabs // 2, SUB, LANES), f32),
            jax.ShapeDtypeStruct((steps, SUB, LANES), f32),
            jax.ShapeDtypeStruct((steps, SUB, LANES), f32),
        ],
        scratch_shapes=[
            pltpu.VMEM((slabs, SUB, LANES), f32),
            pltpu.VMEM((slabs, SUB, LANES), f32),
            pltpu.VMEM((slabs // 2, SUB, LANES), f32),
            pltpu.VMEM((steps, SUB, LANES), f32),
            pltpu.VMEM((steps, SUB, LANES), f32),
            pltpu.SemaphoreType.DMA((5, steps)),
            pltpu.SemaphoreType.DMA((5, steps)),
        ],
        compiler_params=pltpu.CompilerParams(collective_id=0, has_side_effects=True),
        name="local",
    )(u, m, face_map, jnp.asarray(fwd_op), jnp.asarray(bwd_op), jnp.asarray(consts))
    out = pl.pallas_call(
        functools.partial(finish_kernel, sbf, sb, slabs, peers),
        grid=(slabs // sbf,),
        in_specs=[
            pl.BlockSpec(memory_space=pltpu.SMEM),
            pl.BlockSpec((sbf * 64, LANES), lambda i: (i, 0)),
            pl.BlockSpec((sbf, LANES), lambda i: (i, 0)),
            whole((slabs, SUB, LANES)),
            whole((slabs, SUB, LANES)),
            stack(sbf // 2),
            whole((steps, SUB, LANES)),
            whole((steps, SUB, LANES)),
        ],
        out_specs=pl.BlockSpec((sbf * 64, LANES), lambda i: (i, 0)),
        out_shape=jax.ShapeDtypeStruct((slabs * 64, LANES), f32),
        scratch_shapes=[pltpu.SMEM((2, slabs), jnp.int32)],
        name="finish",
    )(slab_ids, v, face_map, pr, plf, z, er, el)
    out = out.reshape(slabs, EZ, 4, EY, LANES).transpose(0, 1, 3, 2, 4)
    return out.reshape(1, slabs, EZ, EY, PTS)


def solution(mesh):
    return jax.shard_map(
        functools.partial(body, SB, SBF, mesh.shape["slab"]),
        mesh=mesh,
        in_specs=(
            P("layer", "slab", None, None, None),
            P("layer", "slab", None, None, None, None),
            P(),
            P("slab", None),
        ),
        out_specs=P("layer", "slab", None, None, None),
        check_vma=False,
    )
```
